32 devices in a mesh: tm: 32 (over z, y, x, core), chan: 1.
Axes of the slice: x: 2, y: 2, z: 4, core: 2. Of those that a mesh axis runs over, the one named last changes fastest.
Arguments:
- signal: bfloat16 [3, 4096, 512], P(None, 'tm', 'chan'), may hold values from -6 to 6
- taps: float32 [10, 2, 512], P(None, None, 'chan'), may hold values from -3 to 3
- w_gate: bfloat16 [10, 512, 2, 512], P(None, None, None, 'chan'), may hold values from -0.25 to 0.25
- w_res: bfloat16 [10, 512, 512], P(None, None, 'chan'), may hold values from -0.25 to 0.25
- w_skip: bfloat16 [10, 512, 512], P(None, None, 'chan'), may hold values from -0.1875 to 0.1875
Outputs:
- stream: bfloat16 [3, 4096, 512], P(None, 'tm', 'chan')
- skips: bfloat16 [3, 4096, 512], P(None, 'tm', 'chan')
The draws below stay inside these ranges and needn't reach their ends.
All inputs are finite; a program needn't handle non-finite values.
Results may differ from the reference program's by a relative error of at most 0.02.
Values may be sent and summed in bfloat16 or wider, within the bound.
A program may use at most 64 MiB of HBM per device.

```python
import jax
import jax.numpy as jnp

C = 512
LAYERS = 10
SEQS = 3
LEN = 4096


def level_of(rng, extent, pieces, low, high):
    gain, own = 1.0, jax.random.fold_in(rng, 6)
    for dim, parts in pieces:
        draws = jnp.exp(jax.random.uniform(jax.random.fold_in(own, dim), (parts,), jnp.float32, low / len(pieces), high / len(pieces)))
        gain = gain * jnp.repeat(draws, extent[dim] // parts).reshape([-1 if axis == dim else 1 for axis in range(len(extent))])
    return gain


def noise(rng, dims, deviation, most, pieces=(), held_as=jnp.bfloat16):
    drawn = jax.random.normal(rng, dims, jnp.float32) * deviation
    if len(pieces) > 0:
        drawn = level_of(rng, dims, pieces, -0.22, 0.18) * drawn
    return jnp.clip(drawn, min=-most, max=most).astype(held_as)


def setup_inputs(seed: int = 0) -> dict:
    streams_of = jax.random.split(jax.random.key(seed), 6)
    signal = noise(streams_of[0], (SEQS, LEN, C), 1.0, 6.0, ((1, 32),))
    taps = noise(streams_of[1], (LAYERS, 2, C), 0.8, 3.0, (), jnp.float32)
    w_gate = noise(streams_of[2], (LAYERS, C, 2, C), C ** -0.5, 0.25)
    w_res = noise(streams_of[3], (LAYERS, C, C), C ** -0.5, 0.25)
    w_skip = noise(streams_of[4], (LAYERS, C, C), (C * 2) ** -0.5, 0.1875)
    return {"signal": signal, "taps": taps, "w_gate": w_gate, "w_res": w_res, "w_skip": w_skip}


def reference(signal, taps, w_gate, w_res, w_skip):
    stream = signal
    skip = jnp.zeros((SEQS, LEN, C), jnp.float32)
    for layer in range(LAYERS):
        delay = 2 ** layer
        delayed = jnp.concatenate([jnp.zeros((SEQS, delay, C), jnp.bfloat16), stream[:, :LEN - delay]], axis=1)
        conv = (taps[layer, 0] * delayed.astype(jnp.float32) + taps[layer, 1] * stream.astype(jnp.float32)).astype(jnp.bfloat16)
        hidden = jnp.einsum("stc,cko->stko", conv.astype(jnp.float32), w_gate[layer].astype(jnp.float32))
        gated = (jnp.tanh(hidden[:, :, 0]) * jax.nn.sigmoid(hidden[:, :, 1])).astype(jnp.bfloat16)
        gated_f = gated.astype(jnp.float32)
        stream = (stream.astype(jnp.float32) + jnp.einsum("stc,co->sto", gated_f, w_res[layer].astype(jnp.float32))).astype(jnp.bfloat16)
        skip = skip + jnp.einsum("stc,co->sto", gated_f, w_skip[layer].astype(jnp.float32))
    return stream, skip.astype(jnp.bfloat16)
```

```python
import functools

import jax
import jax.numpy as jnp
from jax import lax
from jax.experimental import pallas as pl
from jax.experimental.pallas import tpu as pltpu
from jax.sharding import PartitionSpec as P

MESH = pl.DeviceIdType.MESH
BF16, F32 = jnp.bfloat16, jnp.float32
ALIGN = 16
VMEM_LIMIT = 60 * 1024 * 1024


def shifted(value, axis, steps):
    count = lax.axis_size(axis)
    leading, last = (max(0, -steps), min(count, count - steps))
    return lax.ppermute(value, axis, [(source, source + steps) for source in range(leading, last)])


def delay_block(stream, delay, near_fn, far_fn):
    length = stream.shape[1]
    whole, rest = divmod(delay, length)
    if whole == 0:
        nearer = stream
    else:
        nearer = near_fn(stream, whole)
    if rest == 0:
        return nearer
    farther = far_fn(stream[:, length - rest :], whole + 1)
    return jnp.concatenate([farther, nearer[:, : length - rest]], axis=1)


def near_time(block, steps):
    return shifted(block, "tm", steps)


def far_time(block, steps):
    return shifted(block, "tm", steps)


def gate_units(hidden):
    return (jnp.tanh(hidden[:, :, 0]) * jax.nn.sigmoid(hidden[:, :, 1])).astype(jnp.bfloat16)


def local(signal, taps, w_gate, w_res, w_skip):
    stream = signal
    seqs, length, local_c = stream.shape
    skip = jnp.zeros((seqs, length, local_c), jnp.float32)
    for layer in range(taps.shape[0]):
        delayed = delay_block(stream, 2**layer, near_time, far_time)
        conv = (
            taps[layer, 0] * delayed.astype(jnp.float32)
            + taps[layer, 1] * stream.astype(jnp.float32)
        ).astype(jnp.bfloat16)
        gate_w = w_gate[layer]
        hidden = jnp.einsum(
            "stc,cko->stko",
            lax.all_gather(conv, "chan", axis=2, tiled=True),
            gate_w,
            preferred_element_type=jnp.float32,
        )
        gated = gate_units(hidden)
        res_w = w_res[layer]
        skip_w = w_skip[layer]
        piece = lax.all_gather(gated, "chan", axis=2, tiled=True)
        update = jnp.einsum("stc,co->sto", piece, res_w, preferred_element_type=jnp.float32)
        skip_part = jnp.einsum("stc,co->sto", piece, skip_w, preferred_element_type=jnp.float32)
        stream = (stream.astype(jnp.float32) + update).astype(jnp.bfloat16)
        skip = skip + skip_part
    return (stream, skip.astype(jnp.bfloat16))


def tanh_gate(filt, gate):
    return (jnp.tanh(filt) * (0.5 * jnp.tanh(0.5 * gate) + 0.5)).astype(BF16)


def kernel(n, layers, near, sig, taps, wg_hbm, wr_hbm, ws_hbm, out_x, out_skip, *scratch):
    wg, wr, ws, xs, skip, w_sem, send_sem, recv_sem = scratch[:8]
    halos = scratch[8:]
    seqs, length, width = sig.shape
    me = lax.axis_index("tm")
    clean = near - 1
    steps = [max(1, 2**layer // length) for layer in range(layers)]
    reach = sorted(set(steps))
    rows_of = [min(length, max(ALIGN, 2**layer)) for layer in range(layers)]
    half = min(256, width)

    def weights(layer):
        return [
            pltpu.make_async_copy(wg_hbm.at[layer], wg.at[layer], w_sem.at[layer, 0]),
            pltpu.make_async_copy(wr_hbm.at[layer], wr.at[layer], w_sem.at[layer, 1]),
            pltpu.make_async_copy(ws_hbm.at[layer], ws.at[layer], w_sem.at[layer, 2]),
        ]

    for layer in range(layers):
        for copy in weights(layer):
            copy.start()

    barrier = pltpu.get_barrier_semaphore()
    for step in reach:
        for ok, other in ((me + step < n, me + step), (me >= step, me - step)):

            @pl.when(ok)
            def _(other=other):
                pl.semaphore_signal(barrier, inc=1, device_id={"tm": other}, device_id_type=MESH)

    def source(layer):
        return sig if layer == 0 else xs.at[layer - 1]

    def send(layer, s):
        rows = rows_of[layer]
        return pltpu.make_async_remote_copy(
            src_ref=source(layer).at[s, pl.ds(length - rows, rows)],
            dst_ref=halos[layer].at[s],
            send_sem=send_sem.at[layer, s],
            recv_sem=recv_sem.at[layer, s],
            device_id={"tm": me + steps[layer]},
            device_id_type=MESH,
        )

    def start_send(layer, which):
        @pl.when(me + steps[layer] < n)
        def _():
            for s in which:
                send(layer, s).start()

    def take(layer, which):
        @pl.when(me >= steps[layer])
        def _():
            for s in which:
                send(layer, s).wait_recv()

        @pl.when(me < steps[layer])
        def _():
            for s in which:
                halos[layer][s] = jnp.zeros(halos[layer].shape[1:], BF16)

    def load(layer, s, low, high):
        return source(layer)[s, low:high]

    def finish(layer, delayed, own, which, low, high, fresh=False):
        count = high - low
        own_f = jnp.concatenate(own, axis=0).astype(F32) if len(own) > 1 else own[0].astype(F32)
        late = jnp.concatenate(delayed, axis=0) if len(delayed) > 1 else delayed[0]
        conv = (taps[layer, 0:1] * late.astype(F32) + taps[layer, 1:2] * own_f).astype(BF16)
        parts = []
        for at in range(0, width, half):
            filt = jnp.dot(conv, wg[layer, 0, :, at : at + half], preferred_element_type=F32)
            gate = jnp.dot(conv, wg[layer, 1, :, at : at + half], preferred_element_type=F32)
            parts.append(tanh_gate(filt, gate))
        z = jnp.concatenate(parts, axis=1) if len(parts) > 1 else parts[0]
        last = layer == layers - 1
        for at in range(0, width, half):
            cols = slice(at, at + half)
            update = jnp.dot(z, wr[layer, :, cols], preferred_element_type=F32)
            new = (own_f[:, cols] + update).astype(BF16)
            for i, s in enumerate(which):
                part = new[i * count : (i + 1) * count]
                if last:
                    out_x[s, low:high, cols] = part
                else:
                    xs[layer, s, low:high, cols] = part
        if not last:
            yield
        for at in range(0, width, half):
            cols = slice(at, at + half)
            more = jnp.dot(z, ws[layer, :, cols], preferred_element_type=F32)
            for i, s in enumerate(which):
                part = more[i * count : (i + 1) * count]
                if not fresh:
                    part = skip[s, low:high, cols] + part
                if last:
                    out_skip[s, low:high, cols] = part.astype(BF16)
                else:
                    skip[s, low:high, cols] = part
        if last:
            yield

    every = list(range(seqs))
    top = [max(ALIGN, 2 ** (layer + 1)) for layer in range(clean)]
    first = [0 if 2 ** (layer + 2) <= ALIGN * 1 else 0 for layer in range(clean)]
    for layer in range(clean - 1, -1, -1):
        need = top[layer] if layer == clean - 1 else first[layer + 1] - 2 ** (layer + 1)
        first[layer] = max(0, min(need, top[layer]) // ALIGN * ALIGN)

    for layer in range(clean):
        delay, low = 2**layer, first[layer]
        for copy in weights(layer):
            copy.wait()
        delayed, own = [], []
        for s in every:
            if delay < ALIGN:
                begin = max(0, low - ALIGN)
                block = pltpu.roll(load(layer, s, begin, length).astype(F32), delay, 0)
                delayed.append(block[low - begin :])
            else:
                delayed.append(load(layer, s, low - delay, length - delay))
            own.append(load(layer, s, low, length))
        work = finish(layer, delayed, own, every, low, length, fresh=layer == 0)
        next(work)
        if layer == 0:
            total = sum(((me + step < n).astype(jnp.int32) + (me >= step).astype(jnp.int32)) for step in reach)
            pl.semaphore_wait(barrier, total)
            start_send(0, every)
        start_send(layer + 1, every)
        for _ in work:
            pass

    for layer in range(clean):
        delay, high = 2**layer, top[layer]
        take(layer, every)
        delayed, own = [], []
        for s in every:
            rows = rows_of[layer]
            tail = halos[layer][s]
            if delay < ALIGN:
                joined = jnp.concatenate([tail.astype(F32), load(layer, s, 0, high).astype(F32)], axis=0)
                delayed.append(pltpu.roll(joined, delay, 0)[rows:])
            else:
                delayed.append(jnp.concatenate([tail, load(layer, s, 0, high - delay)], axis=0))
            own.append(load(layer, s, 0, high))
        for _ in finish(layer, delayed, own, every, 0, high, fresh=layer == 0):
            pass

    for layer in range(clean, layers):
        for copy in weights(layer):
            copy.wait()
        for s in every:
            take(layer, [s])
            late = halos[layer][s]
            if 2**layer < length:
                late = jnp.concatenate([late, load(layer, s, 0, length - 2**layer)], axis=0)
            work = finish(layer, [late], [load(layer, s, 0, length)], [s], 0, length)
            next(work)
            if layer + 1 < layers:
                start_send(layer + 1, [s])
            for _ in work:
                pass

    for layer in range(layers):

        @pl.when(me + steps[layer] < n)
        def _(layer=layer):
            for s in every:
                send(layer, s).wait_send()


def fused(n, signal, taps, w_gate, w_res, w_skip):
    seqs, length, width = signal.shape
    layers = taps.shape[0]
    near = length.bit_length() - 1
    halves = jnp.transpose(w_gate, (0, 2, 1, 3))
    halos = [
        pltpu.VMEM((seqs, min(length, max(ALIGN, 2**layer)), width), BF16) for layer in range(layers)
    ]
    flops = 2 * seqs * length * width * width * 4 * layers
    in_vmem, anywhere = pl.BlockSpec(memory_space=pltpu.VMEM), pl.BlockSpec(memory_space=pl.ANY)
    return pl.pallas_call(
        functools.partial(kernel, n, layers, near),
        out_shape=[jax.ShapeDtypeStruct(signal.shape, BF16)] * 2,
        in_specs=[in_vmem, in_vmem, anywhere, anywhere, anywhere],
        out_specs=[in_vmem, in_vmem],
        scratch_shapes=[
            pltpu.VMEM((layers, 2, width, width), BF16),
            pltpu.VMEM((layers, width, width), BF16),
            pltpu.VMEM((layers, width, width), BF16),
            pltpu.VMEM((layers - 1, seqs, length, width), BF16),
            pltpu.VMEM((seqs, length, width), F32),
            pltpu.SemaphoreType.DMA((layers, 3)),
            pltpu.SemaphoreType.DMA((layers, seqs)),
            pltpu.SemaphoreType.DMA((layers, seqs)),
            *halos,
        ],
        compiler_params=pltpu.CompilerParams(collective_id=0, has_side_effects=True, vmem_limit_bytes=VMEM_LIMIT),
        cost_estimate=pl.CostEstimate(flops=flops, bytes_accessed=8 * layers * width * width, transcendentals=0),
        name="stack",
    )(signal, taps, halves, w_res, w_skip)


def solution(mesh):
    in_specs = (
        P(None, "tm", "chan"),
        P(None, None, "chan"),
        P(None, None, None, "chan"),
        P(None, None, "chan"),
        P(None, None, "chan"),
    )
    out_specs = (P(None, "tm", "chan"), P(None, "tm", "chan"))

    def body(*args):
        length, layers = args[0].shape[1], args[1].shape[0]
        power = length & (length - 1) == 0 and length >= 4 * ALIGN and 2 ** (layers - 1) >= length
        if mesh.shape["chan"] == 1 and power:
            return tuple(fused(mesh.shape["tm"], *args))
        return local(*args)

    return jax.shard_map(body, mesh=mesh, in_specs=in_specs, out_specs=out_specs, check_vma=False)
```

```python
import functools

import jax
import jax.numpy as jnp
from jax import lax
from jax.experimental import pallas as pl
from jax.experimental.pallas import tpu as pltpu
from jax.sharding import PartitionSpec as P

MESH = pl.DeviceIdType.MESH
BF16, F32 = jnp.bfloat16, jnp.float32
ALIGN = 16
VMEM_LIMIT = 56000 * 1024


def shifted(value, axis, steps):
    count = lax.axis_size(axis)
    leading, last = (max(0, -steps), min(count, count - steps))
    return lax.ppermute(value, axis, [(source, source + steps) for source in range(leading, last)])


def delay_block(stream, delay, near_fn, far_fn):
    length = stream.shape[1]
    whole, rest = divmod(delay, length)
    if whole == 0:
        nearer = stream
    else:
        nearer = near_fn(stream, whole)
    if rest == 0:
        return nearer
    farther = far_fn(stream[:, length - rest :], whole + 1)
    return jnp.concatenate([farther, nearer[:, : length - rest]], axis=1)


def near_time(block, steps):
    return shifted(block, "tm", steps)


def far_time(block, steps):
    return shifted(block, "tm", steps)


def gate_units(hidden):
    return (jnp.tanh(hidden[:, :, 0]) * jax.nn.sigmoid(hidden[:, :, 1])).astype(jnp.bfloat16)


def local(signal, taps, w_gate, w_res, w_skip):
    stream = signal
    seqs, length, local_c = stream.shape
    skip = jnp.zeros((seqs, length, local_c), jnp.float32)
    for layer in range(taps.shape[0]):
        delayed = delay_block(stream, 2**layer, near_time, far_time)
        conv = (
            taps[layer, 0] * delayed.astype(jnp.float32)
            + taps[layer, 1] * stream.astype(jnp.float32)
        ).astype(jnp.bfloat16)
        gate_w = w_gate[layer]
        hidden = jnp.einsum(
            "stc,cko->stko",
            lax.all_gather(conv, "chan", axis=2, tiled=True),
            gate_w,
            preferred_element_type=jnp.float32,
        )
        gated = gate_units(hidden)
        res_w = w_res[layer]
        skip_w = w_skip[layer]
        piece = lax.all_gather(gated, "chan", axis=2, tiled=True)
        update = jnp.einsum("stc,co->sto", piece, res_w, preferred_element_type=jnp.float32)
        skip_part = jnp.einsum("stc,co->sto", piece, skip_w, preferred_element_type=jnp.float32)
        stream = (stream.astype(jnp.float32) + update).astype(jnp.bfloat16)
        skip = skip + skip_part
    return (stream, skip.astype(jnp.bfloat16))


def tanh_gate(filt, gate):
    return (jnp.tanh(filt) * (0.5 * jnp.tanh(0.5 * gate) + 0.5)).astype(BF16)


def split_pairs(pairs, out):
    width = pairs.shape[0]
    block = min(128, width)
    row = lax.broadcasted_iota(jnp.int32, (2 * block, 2 * block), 0)
    column = lax.broadcasted_iota(jnp.int32, (2 * block, 2 * block), 1)
    wanted = jnp.where(row < block, 2 * row, 2 * (row - block) + 1)
    order = jnp.where(column == wanted, 1.0, 0.0).astype(F32).astype(BF16)
    for at in range(0, width, block):
        both = pairs[at : at + block].reshape(2 * block, pairs.shape[2])
        sorted_rows = jnp.dot(order, both, preferred_element_type=F32).astype(BF16)
        out[0, at : at + block] = sorted_rows[:block]
        out[1, at : at + block] = sorted_rows[block:]


def kernel(n, layers, near, sig_hbm, taps_hbm, wg_hbm, wr_hbm, ws_hbm, out_x, out_skip, *scratch):
    sig, taps, raw, wg, wr, ws, xs, skip, in_sem, w_sem, send_sem, recv_sem = scratch[:12]
    halos = scratch[12:]
    seqs, length, width = sig.shape
    me = lax.axis_index("tm")
    clean = near - 1
    steps = [max(1, 2**layer // length) for layer in range(layers)]
    reach = sorted(set(steps))
    rows_of = [min(length, max(ALIGN, 2**layer)) for layer in range(layers)]
    half = min(256, width)

    def weights(layer):
        return [
            pltpu.make_async_copy(wg_hbm.at[layer], raw.at[layer], w_sem.at[layer, 0]),
            pltpu.make_async_copy(wr_hbm.at[layer], wr.at[layer], w_sem.at[layer, 1]),
            pltpu.make_async_copy(ws_hbm.at[layer], ws.at[layer], w_sem.at[layer, 2]),
        ]

    inputs = [
        pltpu.make_async_copy(sig_hbm, sig, in_sem.at[0]),
        pltpu.make_async_copy(taps_hbm, taps, in_sem.at[1]),
    ]
    for copy in inputs:
        copy.start()
    for layer in range(layers):
        for copy in weights(layer):
            copy.start()

    barrier = pltpu.get_barrier_semaphore()
    for step in reach:
        for ok, other in ((me + step < n, me + step), (me >= step, me - step)):

            @pl.when(ok)
            def _(other=other):
                pl.semaphore_signal(barrier, inc=1, device_id={"tm": other}, device_id_type=MESH)

    def source(layer):
        return sig if layer == 0 else xs.at[layer - 1]

    def send(layer, s):
        rows = rows_of[layer]
        return pltpu.make_async_remote_copy(
            src_ref=source(layer).at[s, pl.ds(length - rows, rows)],
            dst_ref=halos[layer].at[s],
            send_sem=send_sem.at[layer, s],
            recv_sem=recv_sem.at[layer, s],
            device_id={"tm": me + steps[layer]},
            device_id_type=MESH,
        )

    def start_send(layer, which):
        @pl.when(me + steps[layer] < n)
        def _():
            for s in which:
                send(layer, s).start()

    def take(layer, which):
        @pl.when(me >= steps[layer])
        def _():
            for s in which:
                send(layer, s).wait_recv()

        @pl.when(me < steps[layer])
        def _():
            for s in which:
                halos[layer][s] = jnp.zeros(halos[layer].shape[1:], BF16)

    def load(layer, s, low, high):
        return source(layer)[s, low:high]

    def finish(layer, delayed, own, which, low, high, fresh=False):
        count = high - low
        own_f = jnp.concatenate(own, axis=0).astype(F32) if len(own) > 1 else own[0].astype(F32)
        late = jnp.concatenate(delayed, axis=0) if len(delayed) > 1 else delayed[0]
        conv = (taps[layer, 0:1] * late.astype(F32) + taps[layer, 1:2] * own_f).astype(BF16)
        parts = []
        for at in range(0, width, half):
            filt = jnp.dot(conv, wg[layer, 0, :, at : at + half], preferred_element_type=F32)
            gate = jnp.dot(conv, wg[layer, 1, :, at : at + half], preferred_element_type=F32)
            parts.append(tanh_gate(filt, gate))
        z = jnp.concatenate(parts, axis=1) if len(parts) > 1 else parts[0]
        last = layer == layers - 1
        for at in range(0, width, half):
            cols = slice(at, at + half)
            update = jnp.dot(z, wr[layer, :, cols], preferred_element_type=F32)
            new = (own_f[:, cols] + update).astype(BF16)
            for i, s in enumerate(which):
                part = new[i * count : (i + 1) * count]
                if last:
                    out_x[s, low:high, cols] = part
                else:
                    xs[layer, s, low:high, cols] = part
        if not last:
            yield
        for at in range(0, width, half):
            cols = slice(at, at + half)
            more = jnp.dot(z, ws[layer, :, cols], preferred_element_type=F32)
            for i, s in enumerate(which):
                part = more[i * count : (i + 1) * count]
                if not fresh:
                    part = skip[s, low:high, cols] + part
                if last:
                    out_skip[s, low:high, cols] = part.astype(BF16)
                else:
                    skip[s, low:high, cols] = part
        if last:
            yield

    every = list(range(seqs))
    top = [max(ALIGN, 2 ** (layer + 1)) for layer in range(clean)]
    first = [0 if 2 ** (layer + 2) <= ALIGN * 1 else 0 for layer in range(clean)]
    for layer in range(clean - 1, -1, -1):
        need = top[layer] if layer == clean - 1 else first[layer + 1] - 2 ** (layer + 1)
        first[layer] = max(0, min(need, top[layer]) // ALIGN * ALIGN)

    for copy in inputs:
        copy.wait()
    for layer in range(clean):
        delay, low = 2**layer, first[layer]
        for copy in weights(layer):
            copy.wait()
        split_pairs(raw.at[layer], wg.at[layer])
        delayed, own = [], []
        for s in every:
            if delay < ALIGN:
                begin = max(0, low - ALIGN)
                block = pltpu.roll(load(layer, s, begin, length).astype(F32), delay, 0)
                delayed.append(block[low - begin :])
            else:
                delayed.append(load(layer, s, low - delay, length - delay))
            own.append(load(layer, s, low, length))
        work = finish(layer, delayed, own, every, low, length, fresh=layer == 0)
        next(work)
        if layer == 0:
            total = sum(((me + step < n).astype(jnp.int32) + (me >= step).astype(jnp.int32)) for step in reach)
            pl.semaphore_wait(barrier, total)
            start_send(0, every)
        start_send(layer + 1, every)
        for _ in work:
            pass

    def arrive(layer):
        for copy in weights(layer):
            copy.wait()
        split_pairs(raw.at[layer], wg.at[layer])

    arrive(clean)

    for layer in range(clean):
        delay, high = 2**layer, top[layer]
        take(layer, every)
        delayed, own = [], []
        for s in every:
            rows = rows_of[layer]
            tail = halos[layer][s]
            if delay < ALIGN:
                joined = jnp.concatenate([tail.astype(F32), load(layer, s, 0, high).astype(F32)], axis=0)
                delayed.append(pltpu.roll(joined, delay, 0)[rows:])
            else:
                delayed.append(jnp.concatenate([tail, load(layer, s, 0, high - delay)], axis=0))
            own.append(load(layer, s, 0, high))
        for _ in finish(layer, delayed, own, every, 0, high, fresh=layer == 0):
            pass

    for layer in range(clean, layers):
        if layer == clean + 1:
            for later in range(layer, layers):
                arrive(later)
        for s in every:
            take(layer, [s])
            late = halos[layer][s]
            if 2**layer < length:
                late = jnp.concatenate([late, load(layer, s, 0, length - 2**layer)], axis=0)
            work = finish(layer, [late], [load(layer, s, 0, length)], [s], 0, length)
            next(work)
            if layer + 1 < layers:
                start_send(layer + 1, [s])
            for _ in work:
                pass

    for layer in range(layers):

        @pl.when(me + steps[layer] < n)
        def _(layer=layer):
            for s in every:
                send(layer, s).wait_send()


def fused(n, signal, taps, w_gate, w_res, w_skip):
    seqs, length, width = signal.shape
    layers = taps.shape[0]
    near = length.bit_length() - 1
    halos = [
        pltpu.VMEM((seqs, min(length, max(ALIGN, 2**layer)), width), BF16) for layer in range(layers)
    ]
    flops = 2 * seqs * length * width * width * 4 * layers
    in_vmem, anywhere = pl.BlockSpec(memory_space=pltpu.VMEM), pl.BlockSpec(memory_space=pl.ANY)
    return pl.pallas_call(
        functools.partial(kernel, n, layers, near),
        out_shape=[pltpu.VMEM(signal.shape, BF16)] * 2,
        in_specs=[anywhere] * 5,
        out_specs=[in_vmem, in_vmem],
        scratch_shapes=[
            pltpu.VMEM(signal.shape, BF16),
            pltpu.VMEM(taps.shape, F32),
            pltpu.VMEM((layers, width, 2, width), BF16),
            pltpu.VMEM((layers, 2, width, width), BF16),
            pltpu.VMEM((layers, width, width), BF16),
            pltpu.VMEM((layers, width, width), BF16),
            pltpu.VMEM((layers - 1, seqs, length, width), BF16),
            pltpu.VMEM((seqs, length, width), F32),
            pltpu.SemaphoreType.DMA((2,)),
            pltpu.SemaphoreType.DMA((layers, 3)),
            pltpu.SemaphoreType.DMA((layers, seqs)),
            pltpu.SemaphoreType.DMA((layers, seqs)),
            *halos,
        ],
        compiler_params=pltpu.CompilerParams(collective_id=0, has_side_effects=True, vmem_limit_bytes=VMEM_LIMIT),
        cost_estimate=pl.CostEstimate(flops=flops, bytes_accessed=8 * layers * width * width, transcendentals=0),
        name="stack",
    )(signal, taps, w_gate, w_res, w_skip)


def solution(mesh):
    in_specs = (
        P(None, "tm", "chan"),
        P(None, None, "chan"),
        P(None, None, None, "chan"),
        P(None, None, "chan"),
        P(None, None, "chan"),
    )
    out_specs = (P(None, "tm", "chan"), P(None, "tm", "chan"))

    def body(*args):
        length, layers = args[0].shape[1], args[1].shape[0]
        power = length & (length - 1) == 0 and length >= 4 * ALIGN and 2 ** (layers - 1) >= length
        if mesh.shape["chan"] == 1 and power:
            return tuple(fused(mesh.shape["tm"], *args))
        return local(*args)

    return jax.shard_map(body, mesh=mesh, in_specs=in_specs, out_specs=out_specs, check_vma=False)
```

```python
import functools

import jax
import jax.numpy as jnp
from jax import lax
from jax.experimental import pallas as pl
from jax.experimental.pallas import tpu as pltpu
from jax.sharding import PartitionSpec as P

MESH = pl.DeviceIdType.MESH
BF16, F32 = jnp.bfloat16, jnp.float32
ALIGN = 16
VMEM_LIMIT = 56000 * 1024


def shifted(value, axis, steps):
    count = lax.axis_size(axis)
    leading, last = (max(0, -steps), min(count, count - steps))
    return lax.ppermute(value, axis, [(source, source + steps) for source in range(leading, last)])


def delay_block(stream, delay, near_fn, far_fn):
    length = stream.shape[1]
    whole, rest = divmod(delay, length)
    if whole == 0:
        nearer = stream
    else:
        nearer = near_fn(stream, whole)
    if rest == 0:
        return nearer
    farther = far_fn(stream[:, length - rest :], whole + 1)
    return jnp.concatenate([farther, nearer[:, : length - rest]], axis=1)


def near_time(block, steps):
    return shifted(block, "tm", steps)


def far_time(block, steps):
    return shifted(block, "tm", steps)


def gate_units(hidden):
    return (jnp.tanh(hidden[:, :, 0]) * jax.nn.sigmoid(hidden[:, :, 1])).astype(jnp.bfloat16)


def local(signal, taps, w_gate, w_res, w_skip):
    stream = signal
    seqs, length, local_c = stream.shape
    skip = jnp.zeros((seqs, length, local_c), jnp.float32)
    for layer in range(taps.shape[0]):
        delayed = delay_block(stream, 2**layer, near_time, far_time)
        conv = (
            taps[layer, 0] * delayed.astype(jnp.float32)
            + taps[layer, 1] * stream.astype(jnp.float32)
        ).astype(jnp.bfloat16)
        gate_w = w_gate[layer]
        hidden = jnp.einsum(
            "stc,cko->stko",
            lax.all_gather(conv, "chan", axis=2, tiled=True),
            gate_w,
            preferred_element_type=jnp.float32,
        )
        gated = gate_units(hidden)
        res_w = w_res[layer]
        skip_w = w_skip[layer]
        piece = lax.all_gather(gated, "chan", axis=2, tiled=True)
        update = jnp.einsum("stc,co->sto", piece, res_w, preferred_element_type=jnp.float32)
        skip_part = jnp.einsum("stc,co->sto", piece, skip_w, preferred_element_type=jnp.float32)
        stream = (stream.astype(jnp.float32) + update).astype(jnp.bfloat16)
        skip = skip + skip_part
    return (stream, skip.astype(jnp.bfloat16))


def tanh_gate(filt, gate):
    return (jnp.tanh(filt) * (0.5 * jnp.tanh(0.5 * gate) + 0.5)).astype(BF16)


def split_pairs(pairs, out):
    width = pairs.shape[0]
    block = min(128, width)
    row = lax.broadcasted_iota(jnp.int32, (2 * block, 2 * block), 0)
    column = lax.broadcasted_iota(jnp.int32, (2 * block, 2 * block), 1)
    wanted = jnp.where(row < block, 2 * row, 2 * (row - block) + 1)
    order = jnp.where(column == wanted, 1.0, 0.0).astype(F32).astype(BF16)
    for at in range(0, width, block):
        both = pairs[at : at + block].reshape(2 * block, pairs.shape[2])
        sorted_rows = jnp.dot(order, both, preferred_element_type=F32).astype(BF16)
        out[0, at : at + block] = sorted_rows[:block]
        out[1, at : at + block] = sorted_rows[block:]


def kernel(n, layers, near, sig_hbm, taps_hbm, wg_hbm, wr_hbm, ws_hbm, out_x, out_skip, *scratch):
    sig, taps, raw, wg, wr, ws, xs, zs, skip, in_sem, w_sem, send_sem, recv_sem = scratch[:13]
    halos = scratch[13:]
    seqs, length, width = sig.shape
    me = lax.axis_index("tm")
    clean = near - 1
    held = zs.shape[0]
    steps = [max(1, 2**layer // length) for layer in range(layers)]
    reach = sorted(set(steps))
    rows_of = [min(length, max(ALIGN, 2**layer)) for layer in range(layers)]
    half = min(256, width)

    def weights(layer):
        return [
            pltpu.make_async_copy(wg_hbm.at[layer], raw.at[layer], w_sem.at[layer, 0]),
            pltpu.make_async_copy(wr_hbm.at[layer], wr.at[layer], w_sem.at[layer, 1]),
            pltpu.make_async_copy(ws_hbm.at[layer], ws.at[layer], w_sem.at[layer, 2]),
        ]

    inputs = [
        pltpu.make_async_copy(sig_hbm, sig, in_sem.at[0]),
        pltpu.make_async_copy(taps_hbm, taps, in_sem.at[1]),
    ]
    for copy in inputs:
        copy.start()
    for layer in range(layers):
        for copy in weights(layer):
            copy.start()

    barrier = pltpu.get_barrier_semaphore()
    for step in reach:
        for ok, other in ((me + step < n, me + step), (me >= step, me - step)):

            @pl.when(ok)
            def _(other=other):
                pl.semaphore_signal(barrier, inc=1, device_id={"tm": other}, device_id_type=MESH)

    def source(layer):
        return sig if layer == 0 else xs.at[layer - 1]

    def send(layer, s):
        rows = rows_of[layer]
        return pltpu.make_async_remote_copy(
            src_ref=source(layer).at[s, pl.ds(length - rows, rows)],
            dst_ref=halos[layer].at[s],
            send_sem=send_sem.at[layer, s],
            recv_sem=recv_sem.at[layer, s],
            device_id={"tm": me + steps[layer]},
            device_id_type=MESH,
        )

    def start_send(layer, which):
        @pl.when(me + steps[layer] < n)
        def _():
            for s in which:
                send(layer, s).start()

    def take(layer, which):
        @pl.when(me >= steps[layer])
        def _():
            for s in which:
                send(layer, s).wait_recv()

        @pl.when(me < steps[layer])
        def _():
            for s in which:
                halos[layer][s] = jnp.zeros(halos[layer].shape[1:], BF16)

    def load(layer, s, low, high):
        return source(layer)[s, low:high]

    def finish(layer, delayed, own, which, low, high):
        count = high - low
        own_f = jnp.concatenate(own, axis=0).astype(F32) if len(own) > 1 else own[0].astype(F32)
        late = jnp.concatenate(delayed, axis=0) if len(delayed) > 1 else delayed[0]
        conv = (taps[layer, 0:1] * late.astype(F32) + taps[layer, 1:2] * own_f).astype(BF16)
        parts = []
        for at in range(0, width, half):
            filt = jnp.dot(conv, wg[layer, 0, :, at : at + half], preferred_element_type=F32)
            gate = jnp.dot(conv, wg[layer, 1, :, at : at + half], preferred_element_type=F32)
            parts.append(tanh_gate(filt, gate))
        z = jnp.concatenate(parts, axis=1) if len(parts) > 1 else parts[0]
        last = layer == layers - 1
        if layer < held:
            for i, s in enumerate(which):
                zs[layer, s, low:high] = z[i * count : (i + 1) * count]
        for at in range(0, width, half):
            cols = slice(at, at + half)
            update = jnp.dot(z, wr[layer, :, cols], preferred_element_type=F32)
            new = (own_f[:, cols] + update).astype(BF16)
            for i, s in enumerate(which):
                part = new[i * count : (i + 1) * count]
                if last:
                    out_x[s, low:high, cols] = part
                else:
                    xs[layer, s, low:high, cols] = part
        if not last:
            yield
        if layer < held:
            return
        for at in range(0, width, half):
            cols = slice(at, at + half)
            more = jnp.dot(z, ws[layer, :, cols], preferred_element_type=F32)
            for i, s in enumerate(which):
                part = more[i * count : (i + 1) * count]
                part = skip[s, low:high, cols] + part
                if last:
                    out_skip[s, low:high, cols] = part.astype(BF16)
                else:
                    skip[s, low:high, cols] = part
        if last:
            yield

    every = list(range(seqs))
    top = [max(ALIGN, 2 ** (layer + 1)) for layer in range(clean)]
    first = [0 if 2 ** (layer + 2) <= ALIGN * 1 else 0 for layer in range(clean)]
    for layer in range(clean - 1, -1, -1):
        need = top[layer] if layer == clean - 1 else first[layer + 1] - 2 ** (layer + 1)
        first[layer] = max(0, min(need, top[layer]) // ALIGN * ALIGN)

    for copy in inputs:
        copy.wait()
    for layer in range(clean):
        delay, low = 2**layer, first[layer]
        for copy in weights(layer):
            copy.wait()
        split_pairs(raw.at[layer], wg.at[layer])
        delayed, own = [], []
        for s in every:
            if delay < ALIGN:
                begin = max(0, low - ALIGN)
                block = pltpu.roll(load(layer, s, begin, length).astype(F32), delay, 0)
                delayed.append(block[low - begin :])
            else:
                delayed.append(load(layer, s, low - delay, length - delay))
            own.append(load(layer, s, low, length))
        work = finish(layer, delayed, own, every, low, length)
        next(work)
        if layer == 0:
            total = sum(((me + step < n).astype(jnp.int32) + (me >= step).astype(jnp.int32)) for step in reach)
            pl.semaphore_wait(barrier, total)
            start_send(0, every)
        start_send(layer + 1, every)
        for _ in work:
            pass

    def arrive(layer):
        for copy in weights(layer):
            copy.wait()
        split_pairs(raw.at[layer], wg.at[layer])

    arrive(clean)

    for layer in range(clean):
        delay, high = 2**layer, top[layer]
        take(layer, every)
        delayed, own = [], []
        for s in every:
            rows = rows_of[layer]
            tail = halos[layer][s]
            if delay < ALIGN:
                joined = jnp.concatenate([tail.astype(F32), load(layer, s, 0, high).astype(F32)], axis=0)
                delayed.append(pltpu.roll(joined, delay, 0)[rows:])
            else:
                delayed.append(jnp.concatenate([tail, load(layer, s, 0, high - delay)], axis=0))
            own.append(load(layer, s, 0, high))
        for _ in finish(layer, delayed, own, every, 0, high):
            pass

    for layer in range(clean, layers):
        if layer == clean + 1:
            for later in range(layer, layers):
                arrive(later)
        for s in every:
            take(layer, [s])
            late = halos[layer][s]
            if 2**layer < length:
                late = jnp.concatenate([late, load(layer, s, 0, length - 2**layer)], axis=0)
            work = finish(layer, [late], [load(layer, s, 0, length)], [s], 0, length)
            next(work)
            if layer + 1 < layers:
                start_send(layer + 1, [s])
            for _ in work:
                pass
        if layer == held - 1:
            for at in range(0, width, half):
                total = None
                for before in range(held):
                    gated = zs[before].reshape(seqs * length, width)
                    more = jnp.dot(gated, ws[before, :, at : at + half], preferred_element_type=F32)
                    total = more if total is None else total + more
                skip[:, :, at : at + half] = total.reshape(seqs, length, half)

    for layer in range(layers):

        @pl.when(me + steps[layer] < n)
        def _(layer=layer):
            for s in every:
                send(layer, s).wait_send()


def fused(n, signal, taps, w_gate, w_res, w_skip):
    seqs, length, width = signal.shape
    layers = taps.shape[0]
    near = length.bit_length() - 1
    held = min(near + 1, layers - 1)
    halos = [
        pltpu.VMEM((seqs, min(length, max(ALIGN, 2**layer)), width), BF16) for layer in range(layers)
    ]
    flops = 2 * seqs * length * width * width * 4 * layers
    in_vmem, anywhere = pl.BlockSpec(memory_space=pltpu.VMEM), pl.BlockSpec(memory_space=pl.ANY)
    return pl.pallas_call(
        functools.partial(kernel, n, layers, near),
        out_shape=[pltpu.VMEM(signal.shape, BF16)] * 2,
        in_specs=[anywhere] * 5,
        out_specs=[in_vmem, in_vmem],
        scratch_shapes=[
            pltpu.VMEM(signal.shape, BF16),
            pltpu.VMEM(taps.shape, F32),
            pltpu.VMEM((layers, width, 2, width), BF16),
            pltpu.VMEM((layers, 2, width, width), BF16),
            pltpu.VMEM((layers, width, width), BF16),
            pltpu.VMEM((layers, width, width), BF16),
            pltpu.VMEM((layers - 1, seqs, length, width), BF16),
            pltpu.VMEM((held, seqs, length, width), BF16),
            pltpu.VMEM((seqs, length, width), F32),
            pltpu.SemaphoreType.DMA((2,)),
            pltpu.SemaphoreType.DMA((layers, 3)),
            pltpu.SemaphoreType.DMA((layers, seqs)),
            pltpu.SemaphoreType.DMA((layers, seqs)),
            *halos,
        ],
        compiler_params=pltpu.CompilerParams(collective_id=0, has_side_effects=True, vmem_limit_bytes=VMEM_LIMIT),
        cost_estimate=pl.CostEstimate(flops=flops, bytes_accessed=8 * layers * width * width, transcendentals=0),
        name="stack",
    )(signal, taps, w_gate, w_res, w_skip)


def solution(mesh):
    in_specs = (
        P(None, "tm", "chan"),
        P(None, None, "chan"),
        P(None, None, None, "chan"),
        P(None, None, "chan"),
        P(None, None, "chan"),
    )
    out_specs = (P(None, "tm", "chan"), P(None, "tm", "chan"))

    def body(*args):
        length, layers = args[0].shape[1], args[1].shape[0]
        power = length & (length - 1) == 0 and length >= 4 * ALIGN and 2 ** (layers - 1) >= length
        if mesh.shape["chan"] == 1 and power:
            return tuple(fused(mesh.shape["tm"], *args))
        return local(*args)

    return jax.shard_map(body, mesh=mesh, in_specs=in_specs, out_specs=out_specs, check_vma=False)
```
